32 devices in a mesh: row: 8 (over z, y), col: 4 (over x, core).
Axes of the slice: x: 2, y: 2, z: 4, core: 2. Of those that a mesh axis runs over, the one named last changes fastest.
Arguments:
- expression: bfloat16 [4096, 1024], P(('row', 'col')), as said below
- power_order: int32 [20], replicated, may hold values from 0 to 19, each once
Outputs:
- log_conn: float32 [4096, 20], P(('row', 'col'))
- fit: float32 [20], replicated
- slope: float32 [20], replicated
The draws below stay inside these ranges and needn't reach their ends.
Inputs may be any that keep to these rules, and one draw needn't show every extreme that they name: `expression`: each gene's row has mean zero and unit variance over the samples, up to rounding.
All inputs are finite; a program needn't handle non-finite values.
Results may differ from the reference program's by a relative error of at most 0.0029.
Values may be sent and summed in bfloat16 or wider, within the bound.
No kernel may reach another device: no remote copies, remote signals or barrier semaphores. Data moves between devices by JAX's collectives and lax.ppermute only.
A program may use at most 64 MiB of HBM per device.

```python
import math
import jax
import jax.numpy as jnp
from jax import lax

SAMPLES = 1024
POWERS = 20
BINS = 128
GENES_DEV = 128
GENES = 4096
N_COL = 4


module_count = 192


sub_count = 4


factor_count = 96


def draw_expression(key, part):
    keys = jax.random.split(jax.random.fold_in(key, 11), 9)
    eigen = jax.random.normal(keys[0], (module_count, SAMPLES), jnp.float32)
    sub_eigen = jax.random.normal(keys[1], (module_count * sub_count, SAMPLES), jnp.float32)
    factors = jax.random.normal(keys[2], (factor_count, SAMPLES), jnp.float32)
    choices_three = jax.random.randint(keys[3], (GENES, 3), 0, module_count)
    member = jnp.min(choices_three, axis=1)
    sub_member = member * sub_count + jax.random.randint(keys[4], (GENES,), 0, sub_count)
    module_load = jax.random.uniform(keys[5], (GENES,), jnp.float32, 0.1, 0.8)
    sub_load = jax.random.uniform(keys[6], (GENES,), jnp.float32, 0.1, 0.6)
    loadings = 0.07 * jax.random.normal(keys[7], (GENES, factor_count), jnp.float32)
    noise_weight = jax.random.uniform(keys[8], (GENES,), jnp.float32, 0.4, 1.0)
    noise = jax.random.normal(jax.random.fold_in(keys[8], 3), (GENES, SAMPLES), jnp.float32)
    raw = module_load[:, None] * eigen[member] + sub_load[:, None] * sub_eigen[sub_member]
    raw = raw + jnp.dot(loadings, factors, precision=lax.Precision.HIGHEST) + noise_weight[:, None] * noise
    centered = raw - jnp.mean(raw, axis=1, keepdims=True)
    spread = jnp.sqrt(jnp.mean(centered * centered, axis=1, keepdims=True))
    return (centered / spread).astype(jnp.bfloat16)


def setup_inputs(seed: int = 0) -> dict:
    seeds = jax.random.split(jax.random.key(seed), 3)
    return {
        "expression": draw_expression(jax.random.fold_in(seeds[2], 71), 0),
        "power_order": jax.random.permutation(seeds[1], POWERS).astype(jnp.int32),
    }


def power_sums(rows, partners):
    corr = lax.dot_general(rows, partners, (((1,), (1,)), ((), ())), preferred_element_type=jnp.float32) / SAMPLES
    magnitude = jnp.abs(corr)
    current = magnitude
    sums = []
    for power in range(POWERS):
        sums.append(jnp.sum(current, axis=1))
        current = current * magnitude
    return jnp.stack(sums, axis=1)


def scale_free_fit(hist, log_total):
    centers = jnp.arange(BINS, dtype=jnp.float32) * (log_total / (BINS - 1))
    weight_sum = jnp.sum(hist, axis=1, keepdims=True)
    ylog = jnp.log(hist + 1.0) - log_total
    xmean = jnp.sum(hist * centers[None, :], axis=1, keepdims=True) / weight_sum
    ymean = jnp.sum(hist * ylog, axis=1, keepdims=True) / weight_sum
    xdev = centers[None, :] - xmean
    ydev = ylog - ymean
    sxx = jnp.maximum(jnp.sum(hist * xdev * xdev, axis=1) / weight_sum[:, 0], 0.05)
    syy = jnp.maximum(jnp.sum(hist * ydev * ydev, axis=1) / weight_sum[:, 0], 0.05)
    sxy = jnp.sum(hist * xdev * ydev, axis=1) / weight_sum[:, 0]
    return -sxy * jnp.abs(sxy) / (sxx * syy), sxy / sxx


def soft_hist(log_conn, log_total):
    pos = log_conn * ((BINS - 1) / log_total)
    levels = jnp.arange(BINS, dtype=jnp.float32)
    weights = jnp.maximum(0.0, 1.0 - jnp.abs(pos[:, :, None] - levels[None, None, :]))
    return jnp.sum(weights, axis=0)


def reference(expression, power_order):
    block = GENES_DEV * N_COL
    count = GENES // block
    blocks = expression.reshape(count, block, SAMPLES)
    conn = lax.map(lambda rows: power_sums(rows, expression), blocks).reshape(GENES, POWERS)
    selector = (power_order[:, None] == jnp.arange(POWERS, dtype=jnp.int32)[None, :]).astype(jnp.float32)
    picked = jnp.dot(conn, selector.T, precision=lax.Precision.HIGHEST)
    log_conn = jnp.log(picked)
    log_total = math.log(GENES)
    hist = soft_hist(log_conn, log_total)
    fit, slope = scale_free_fit(hist, log_total)
    return log_conn, fit, slope
```

```python
import functools
import math

import jax
import jax.numpy as jnp
from jax import lax
from jax.experimental import pallas as pl
from jax.experimental.pallas import tpu as pltpu
from jax.sharding import PartitionSpec as P

AXES = ("row", "col")
BINS = 128


def swap(x, mask, count):
    return lax.ppermute(x, AXES, [(i, i ^ mask) for i in range(count)])


def spread(block, masks, count):
    held = {0: block}
    for mask in masks:
        for key in list(held):
            held[key ^ mask] = swap(held[key], mask, count)
    return held


def power_kernel(powers, samples, n_panel, n_partner, *refs):
    panel_refs = refs[:n_panel]
    partner_refs = refs[n_panel : n_panel + n_partner]
    out_ref = refs[n_panel + n_partner]
    genes = panel_refs[0].shape[0]
    totals = {}
    for first in range(0, n_panel, 2):
        group = panel_refs[first : first + 2]
        panel = (
            group[0][...] if len(group) == 1 else jnp.concatenate([r[...] for r in group], axis=0)
        )
        for partner_ref in partner_refs:
            corr = lax.dot_general(
                partner_ref[...],
                panel,
                (((1,), (1,)), ((), ())),
                preferred_element_type=jnp.float32,
            )
            for k in range(len(group)):
                magnitude = jnp.abs(corr[:, k * genes : (k + 1) * genes] * (1.0 / samples))
                current = magnitude
                for power in range(powers):
                    part = jnp.sum(current.reshape(-1, 8, genes), axis=0)
                    slot = (first + k, power)
                    totals[slot] = totals[slot] + part if slot in totals else part
                    if power < powers - 1:
                        current = current * magnitude
    for i in range(n_panel):
        for power in range(powers):
            out_ref[i, power, :] = jnp.sum(totals[i, power], axis=0)


def power_sums(panels, partners, powers, samples):
    genes = panels[0].shape[0]
    outs = []
    for first in range(0, len(partners), 8):
        some = partners[first : first + 8]
        pairs = len(panels) * len(some) * genes * some[0].shape[0]
        outs.append(
            pl.pallas_call(
                functools.partial(power_kernel, powers, samples, len(panels), len(some)),
                out_shape=jax.ShapeDtypeStruct((len(panels), powers, genes), jnp.float32),
                in_specs=[pl.BlockSpec(memory_space=pltpu.VMEM)] * (len(panels) + len(some)),
                out_specs=pl.BlockSpec(memory_space=pltpu.VMEM),
                cost_estimate=pl.CostEstimate(
                    flops=pairs * 2 * samples, bytes_accessed=0, transcendentals=0
                ),
                name="power_sums",
            )(*panels, *some)
        )
    return functools.reduce(jnp.add, outs)


def scale_free_fit(hist, log_total, bins):
    centers = jnp.arange(bins, dtype=jnp.float32) * (log_total / (bins - 1))
    weight_sum = jnp.sum(hist, axis=1, keepdims=True)
    ylog = jnp.log(hist + 1.0) - log_total
    xmean = jnp.sum(hist * centers[None, :], axis=1, keepdims=True) / weight_sum
    ymean = jnp.sum(hist * ylog, axis=1, keepdims=True) / weight_sum
    xdev = centers[None, :] - xmean
    ydev = ylog - ymean
    sxx = jnp.maximum(jnp.sum(hist * xdev * xdev, axis=1) / weight_sum[:, 0], 0.05)
    syy = jnp.maximum(jnp.sum(hist * ydev * ydev, axis=1) / weight_sum[:, 0], 0.05)
    sxy = jnp.sum(hist * xdev * ydev, axis=1) / weight_sum[:, 0]
    return (-sxy * jnp.abs(sxy) / (sxx * syy), sxy / sxx)


def on_device(expression, power_order):
    rows, cols = lax.axis_size("row"), lax.axis_size("col")
    count = rows * cols
    genes, samples = expression.shape
    powers = power_order.shape[0]
    log_total = math.log(genes * count)

    row_masks = [cols << i for i in range(rows.bit_length() - 1)]
    col_masks = [1 << i for i in range(cols.bit_length() - 1)]
    far, near = row_masks[-1], row_masks[:-1]
    panel_masks = [far] + col_masks[1:]
    partner_masks = near[::-1] + col_masks[:1]

    partner = list(spread(expression, partner_masks, count).values())
    panel = spread(expression, panel_masks, count)
    keys = list(panel)
    early = [k for k in keys if not k & far]
    late = [k for k in keys if k & far and k != far]
    conn = {}
    for group in (early, [far], late):
        sums = power_sums([panel[k] for k in group], partner, powers, samples)
        for i, k in enumerate(group):
            conn[k] = sums[i]
    for mask in panel_masks[::-1]:
        stacked = jnp.stack([conn[k] for k in keys])
        other = swap(stacked, mask, count)
        conn = {k: conn[k] + other[keys.index(k ^ mask)] for k in keys}

    selector = (power_order[:, None] == jnp.arange(powers, dtype=jnp.int32)[None, :]).astype(
        jnp.float32
    )
    levels = jnp.arange(BINS, dtype=jnp.float32)
    hists = {}
    log_conn = {}
    for k in keys:
        picked = jnp.dot(selector, conn[k], precision=lax.Precision.HIGHEST)
        log_conn[k] = jnp.log(picked)
        position = log_conn[k] * ((BINS - 1) / log_total)
        weights = jnp.maximum(0.0, 1.0 - jnp.abs(position[:, None, :] - levels[None, :, None]))
        hists[k] = jnp.sum(weights, axis=2)
    for mask in panel_masks:
        hists = {k: hists[k] + hists[k ^ mask] for k in hists if not k & mask}
    hist = hists[0]
    for mask in partner_masks:
        hist = hist + swap(hist, mask, count)
    fit, slope = scale_free_fit(hist, log_total, BINS)
    return (log_conn[0].T, fit, slope)


def solution(mesh):
    placed = (P(AXES, None), P())
    return jax.shard_map(
        on_device,
        mesh=mesh,
        in_specs=placed,
        out_specs=(P(AXES, None), P(), P()),
        check_vma=False,
    )
```

```python
import functools
import math

import jax
import jax.numpy as jnp
from jax import lax
from jax.experimental import pallas as pl
from jax.experimental.pallas import tpu as pltpu
from jax.sharding import PartitionSpec as P


AXES = ("row", "col")
BINS = 128
CHUNK = 8
VMEM = pl.BlockSpec(memory_space=pltpu.VMEM)
SMEM = pl.BlockSpec(memory_space=pltpu.SMEM)
PARAMS = pltpu.CompilerParams(vmem_limit_bytes=16 * 2**20)


def swap(x, mask, count):
    return lax.ppermute(x, AXES, [(i, i ^ mask) for i in range(count)])


def spread(block, masks, count):
    held = {0: block}
    for mask in masks:
        for key in list(held):
            held[key ^ mask] = swap(held[key], mask, count)
    return held


def plan(rows, cols):
    row_masks = [cols << i for i in range(rows.bit_length() - 1)]
    col_masks = [1 << i for i in range(cols.bit_length() - 1)]
    return [row_masks[-1]] + col_masks[1:], row_masks[-2::-1] + col_masks[:1]


def in_vmem(x):
    return pltpu.with_memory_space_constraint(x, pltpu.VMEM)


def pair_sum(values):
    while len(values) > 1:
        values = [a + b for a, b in zip(values[::2], values[1::2])]
    return values[0]


def joined(refs):
    return refs[0][...] if len(refs) == 1 else jnp.concatenate([r[...] for r in refs], axis=0)


def add_powers(panel_refs, partner_refs, total_ref):
    genes, samples = panel_refs[0].shape
    powers = total_ref.shape[1]
    panel = joined(panel_refs)
    many = len(panel_refs) > 1
    groups = [partner_refs] if many else [[ref] for ref in partner_refs]
    begun = False
    for group in groups:
        corr = lax.dot_general(
            joined(group), panel, (((1,), (1,)), ((), ())), preferred_element_type=jnp.float32
        )
        for low in range(0, corr.shape[0], genes):
            for i in range(len(panel_refs)):
                block = corr[low : low + genes, i * genes : (i + 1) * genes]
                magnitude = jnp.abs(block * (1.0 / samples))
                square = magnitude * magnitude
                current = [magnitude, square]
                for power in range(powers):
                    part = jnp.sum(current[power % 2].reshape(-1, 8, genes), axis=0)
                    total_ref[i, power] = total_ref[i, power] + part if begun else part
                    if power + 2 < powers:
                        current[power % 2] = current[power % 2] * square
            begun = True


def power_kernel(n_panel, *refs):
    out_ref, total_ref = refs[-2:]
    add_powers(refs[:n_panel], refs[n_panel:-2], total_ref)
    for i in range(n_panel):
        out_ref[i] = jnp.sum(total_ref[i], axis=1)


def power_sums(panels, partners, powers):
    genes, samples = panels[0].shape
    outs = []
    for first in range(0, len(partners), CHUNK):
        some = partners[first : first + CHUNK]
        flops = len(panels) * len(some) * genes * genes * 2 * samples
        outs.append(
            pl.pallas_call(
                functools.partial(power_kernel, len(panels)),
                out_shape=jax.ShapeDtypeStruct((len(panels), powers, genes), jnp.float32),
                in_specs=[VMEM] * (len(panels) + len(some)),
                out_specs=VMEM,
                scratch_shapes=[pltpu.VMEM((len(panels), powers, 8, genes), jnp.float32)],
                compiler_params=PARAMS,
                cost_estimate=pl.CostEstimate(flops=flops, bytes_accessed=0, transcendentals=0),
                name="power_sums",
            )(*map(in_vmem, panels), *map(in_vmem, some))
        )
    return functools.reduce(jnp.add, outs)


def last_kernel(n_panel, n_partner, parts, slot_ref, *refs):
    part_refs = refs[n_panel + n_partner : -2]
    conn_ref, total_ref = refs[-2:]
    slots = len(parts)
    powers = total_ref.shape[1]
    mine = slot_ref[0]
    add_powers(refs[:n_panel], refs[n_panel : n_panel + n_partner], total_ref)
    for i, where in enumerate(parts):
        slot = jnp.bitwise_xor(mine, i)
        values = [part_refs[a][b] for a, b in where if a is not None]
        values += [jnp.sum(total_ref[b], axis=1) for a, b in where if a is None]
        value = functools.reduce(jnp.add, values)
        for power in range(powers):
            conn_ref[pl.ds(power * slots + slot, 1), :] = value[power : power + 1]


def last_sums(slot, panels, partners, done, parts, powers):
    genes, samples = panels[0].shape
    flops = len(panels) * len(partners) * genes * genes * 2 * samples
    return pl.pallas_call(
        functools.partial(last_kernel, len(panels), len(partners), parts),
        out_shape=jax.ShapeDtypeStruct((powers * len(parts), genes), jnp.float32),
        in_specs=[SMEM] + [VMEM] * (len(panels) + len(partners) + len(done)),
        out_specs=VMEM,
        scratch_shapes=[pltpu.VMEM((len(panels), powers, 8, genes), jnp.float32)],
        compiler_params=PARAMS,
        cost_estimate=pl.CostEstimate(flops=flops, bytes_accessed=0, transcendentals=0),
        name="last_sums",
    )(slot, *map(in_vmem, panels), *map(in_vmem, partners), *map(in_vmem, done))


def hist_kernel(scale, power_ref, slot_ref, conn_ref, other_ref, log_ref, hist_ref, logs, places):
    rows, genes = conn_ref.shape
    powers = log_ref.shape[0]
    slots = rows // powers
    mine = slot_ref[0]
    logs[...] = jnp.log(conn_ref[...] + other_ref[...])
    places[...] = logs[...] * scale
    levels = lax.broadcasted_iota(jnp.int32, (BINS, genes), 0).astype(jnp.float32)
    lane = lax.broadcasted_iota(jnp.int32, (BINS, BINS), 1)
    table = jnp.zeros((BINS, BINS), jnp.float32)
    for t in range(powers):
        first = power_ref[t] * slots
        log_ref[pl.ds(t, 1), :] = logs[pl.ds(first + mine, 1), :]
        weights = pair_sum(
            [
                jnp.maximum(0.0, 1.0 - jnp.abs(places[pl.ds(first + m, 1), :] - levels))
                for m in range(slots)
            ]
        )
        table = jnp.where(lane == t, jnp.sum(weights, axis=1, keepdims=True), table)
    hist_ref[...] = table.T[:powers]


def histogram(power_order, slot, conn, other, scale):
    powers = power_order.shape[0]
    genes = conn.shape[1]
    return pl.pallas_call(
        functools.partial(hist_kernel, scale),
        out_shape=(
            pltpu.VMEM((powers, genes), jnp.float32),
            pltpu.VMEM((powers, BINS), jnp.float32),
        ),
        in_specs=[SMEM, SMEM, VMEM, VMEM],
        out_specs=(VMEM, VMEM),
        scratch_shapes=[pltpu.VMEM(conn.shape, jnp.float32)] * 2,
        compiler_params=PARAMS,
        name="histogram",
    )(power_order, slot, in_vmem(conn), in_vmem(other))


def fit_kernel(log_total, hist_ref, other_ref, fit_ref, slope_ref):
    hist = hist_ref[...] + other_ref[...]
    powers = hist.shape[0]
    lane = lax.broadcasted_iota(jnp.int32, (powers, BINS), 1)
    centers = lane.astype(jnp.float32) * (log_total / (BINS - 1))

    def total(x):
        return jnp.sum(x, axis=1, keepdims=True)

    weight_sum = total(hist)
    ylog = jnp.log(hist + 1.0) - log_total
    xdev = centers - total(hist * centers) / weight_sum
    ydev = ylog - total(hist * ylog) / weight_sum
    sxx = jnp.maximum(total(hist * xdev * xdev) / weight_sum, 0.05)
    syy = jnp.maximum(total(hist * ydev * ydev) / weight_sum, 0.05)
    sxy = total(hist * xdev * ydev) / weight_sum
    own = lax.broadcasted_iota(jnp.int32, (powers, BINS), 0) == lane

    def store(ref, column):
        ref[...] = jnp.sum(jnp.where(own, column, 0.0), axis=0)[:powers]

    store(fit_ref, -sxy * jnp.abs(sxy) / (sxx * syy))
    store(slope_ref, sxy / sxx)


def scale_free_fit(hist, other, log_total):
    powers = hist.shape[0]
    return pl.pallas_call(
        functools.partial(fit_kernel, log_total),
        out_shape=(jax.ShapeDtypeStruct((powers,), jnp.float32),) * 2,
        in_specs=[VMEM, VMEM],
        out_specs=(VMEM, VMEM),
        compiler_params=PARAMS,
        name="scale_free_fit",
    )(in_vmem(hist), in_vmem(other))


def on_device(expression, power_order):
    rows, cols = lax.axis_size("row"), lax.axis_size("col")
    count = rows * cols
    powers = power_order.shape[0]
    log_total = math.log(expression.shape[0] * count)
    panel_masks, partner_masks = plan(rows, cols)
    far, core = panel_masks[0], partner_masks[-1]
    low, sides = partner_masks[0], partner_masks[1:-1]

    partner = spread(expression, partner_masks, count)
    panel = spread(expression, panel_masks, count)
    keys = list(panel)
    front = [k for k in keys if not k & far] + [far]
    rear = [k for k in keys if k not in front]

    index = lax.axis_index(AXES)
    slot = sum(((index // mask) % 2) << i for i, mask in enumerate(panel_masks))
    slot = jnp.reshape(slot, (1,)).astype(jnp.int32)

    relayed = [k for k in partner if bin(k & ~core).count("1") > 1]
    waves = [
        ([0], [0]),
        (front, [core] + sides),
        (front[1:], [0]),
        (front, [k ^ core for k in sides] + [low, low ^ core]),
        (front, relayed),
    ]
    done = []
    parts = {k: [] for k in keys}
    for n, (panels, partners) in enumerate(waves):
        done.append(power_sums([panel[k] for k in panels], [partner[k] for k in partners], powers))
        for i, k in enumerate(panels):
            parts[k].append((n, i))
    everyone = list(partner)
    early, late = everyone[CHUNK:], everyone[:CHUNK]
    if early:
        done.append(power_sums([panel[k] for k in rear], [partner[k] for k in early], powers))
    for i, k in enumerate(rear):
        parts[k] += [(len(done) - 1, i)] * bool(early) + [(None, i)]
    conn = last_sums(
        slot,
        [panel[k] for k in rear],
        [partner[k] for k in late],
        done,
        [parts[k] for k in keys],
        powers,
    )

    for mask in panel_masks[:0:-1]:
        conn = conn + swap(conn, mask, count)
    log_conn, hist = histogram(
        power_order, slot, conn, swap(conn, far, count), (BINS - 1) / log_total
    )
    for mask in partner_masks[:-1]:
        hist = hist + swap(hist, mask, count)
    fit, slope = scale_free_fit(hist, swap(hist, core, count), log_total)
    return (log_conn.T, fit, slope)


def solution(mesh):
    placed = (P(AXES, None), P())
    return jax.shard_map(
        on_device,
        mesh=mesh,
        in_specs=placed,
        out_specs=(P(AXES, None), P(), P()),
        check_vma=False,
    )
```

```python
import functools
import math

import jax
import jax.numpy as jnp
from jax import lax
from jax.experimental import pallas as pl
from jax.experimental.pallas import tpu as pltpu
from jax.sharding import PartitionSpec as P


AXES = ("row", "col")
BINS = 128
CHUNK = 8
VMEM = pl.BlockSpec(memory_space=pltpu.VMEM)
SMEM = pl.BlockSpec(memory_space=pltpu.SMEM)
PARAMS = pltpu.CompilerParams(vmem_limit_bytes=16 * 2**20)


def swap(x, mask, count):
    return lax.ppermute(x, AXES, [(i, i ^ mask) for i in range(count)])


def spread(block, masks, count):
    held = {0: block}
    for mask in masks:
        for key in list(held):
            held[key ^ mask] = swap(held[key], mask, count)
    return held


def plan(rows, cols):
    row_masks = [cols << i for i in range(rows.bit_length() - 1)]
    core, *col_masks = [1 << i for i in range(cols.bit_length() - 1)]
    panel_masks = [row_masks[-1]] + col_masks
    partner_masks = row_masks[-2::-1] + [core]
    return panel_masks, partner_masks


def in_vmem(x):
    return pltpu.with_memory_space_constraint(x, pltpu.VMEM)


def pair_sum(values):
    while len(values) > 1:
        values = [a + b for a, b in zip(values[::2], values[1::2])]
    return values[0]


def joined(refs):
    return refs[0][...] if len(refs) == 1 else jnp.concatenate([r[...] for r in refs], axis=0)


def add_powers(panel_refs, partner_refs, total_ref):
    genes, samples = panel_refs[0].shape
    powers = total_ref.shape[1]
    panel = joined(panel_refs)
    many = len(panel_refs) > 1
    groups = [partner_refs] if many else [[ref] for ref in partner_refs]
    begun = False
    for group in groups:
        corr = lax.dot_general(
            joined(group), panel, (((1,), (1,)), ((), ())), preferred_element_type=jnp.float32
        )
        for low in range(0, corr.shape[0], genes):
            for i in range(len(panel_refs)):
                block = corr[low : low + genes, i * genes : (i + 1) * genes]
                magnitude = jnp.abs(block * (1.0 / samples))
                square = magnitude * magnitude
                current = [magnitude, square]
                for power in range(powers):
                    part = jnp.sum(current[power % 2].reshape(-1, 8, genes), axis=0)
                    total_ref[i, power] = total_ref[i, power] + part if begun else part
                    if power + 2 < powers:
                        current[power % 2] = current[power % 2] * square
            begun = True


def power_kernel(n_panel, *refs):
    out_ref, total_ref = refs[-2:]
    add_powers(refs[:n_panel], refs[n_panel:-2], total_ref)
    for i in range(n_panel):
        out_ref[i] = jnp.sum(total_ref[i], axis=1)


def power_sums(panels, partners, powers):
    genes, samples = panels[0].shape
    outs = []
    for first in range(0, len(partners), CHUNK):
        some = partners[first : first + CHUNK]
        flops = len(panels) * len(some) * genes * genes * 2 * samples
        outs.append(
            pl.pallas_call(
                functools.partial(power_kernel, len(panels)),
                out_shape=jax.ShapeDtypeStruct((len(panels), powers, genes), jnp.float32),
                in_specs=[VMEM] * (len(panels) + len(some)),
                out_specs=VMEM,
                scratch_shapes=[pltpu.VMEM((len(panels), powers, 8, genes), jnp.float32)],
                compiler_params=PARAMS,
                cost_estimate=pl.CostEstimate(flops=flops, bytes_accessed=0, transcendentals=0),
                name="power_sums",
            )(*map(in_vmem, panels), *map(in_vmem, some))
        )
    return functools.reduce(jnp.add, outs)


def last_kernel(n_panel, n_partner, parts, slot_ref, *refs):
    part_refs = refs[n_panel + n_partner : -2]
    conn_ref, total_ref = refs[-2:]
    slots = len(parts)
    powers = total_ref.shape[1]
    mine = slot_ref[0]
    add_powers(refs[:n_panel], refs[n_panel : n_panel + n_partner], total_ref)
    for i, where in enumerate(parts):
        slot = jnp.bitwise_xor(mine, i)
        values = [part_refs[a][b] for a, b in where if a is not None]
        values += [jnp.sum(total_ref[b], axis=1) for a, b in where if a is None]
        value = functools.reduce(jnp.add, values)
        for power in range(powers):
            conn_ref[pl.ds(power * slots + slot, 1), :] = value[power : power + 1]


def last_sums(slot, panels, partners, done, parts, powers):
    genes, samples = panels[0].shape
    flops = len(panels) * len(partners) * genes * genes * 2 * samples
    return pl.pallas_call(
        functools.partial(last_kernel, len(panels), len(partners), parts),
        out_shape=jax.ShapeDtypeStruct((powers * len(parts), genes), jnp.float32),
        in_specs=[SMEM] + [VMEM] * (len(panels) + len(partners) + len(done)),
        out_specs=VMEM,
        scratch_shapes=[pltpu.VMEM((len(panels), powers, 8, genes), jnp.float32)],
        compiler_params=PARAMS,
        cost_estimate=pl.CostEstimate(flops=flops, bytes_accessed=0, transcendentals=0),
        name="last_sums",
    )(slot, *map(in_vmem, panels), *map(in_vmem, partners), *map(in_vmem, done))


def hist_kernel(scale, power_ref, slot_ref, conn_ref, other_ref, log_ref, hist_ref, logs, places):
    rows, genes = conn_ref.shape
    powers = log_ref.shape[0]
    slots = rows // powers
    mine = slot_ref[0]
    logs[...] = jnp.log(conn_ref[...] + other_ref[...])
    places[...] = logs[...] * scale
    levels = lax.broadcasted_iota(jnp.int32, (BINS, genes), 0).astype(jnp.float32)
    lane = lax.broadcasted_iota(jnp.int32, (BINS, BINS), 1)
    table = jnp.zeros((BINS, BINS), jnp.float32)
    for t in range(powers):
        first = power_ref[t] * slots
        log_ref[pl.ds(t, 1), :] = logs[pl.ds(first + mine, 1), :]
        away = pair_sum(
            [
                jnp.minimum(jnp.abs(places[pl.ds(first + m, 1), :] - levels), 1.0)
                for m in range(slots)
            ]
        )
        weights = slots - away
        table = jnp.where(lane == t, jnp.sum(weights, axis=1, keepdims=True), table)
    hist_ref[...] = table.T[:powers]


def histogram(power_order, slot, conn, other, scale):
    powers = power_order.shape[0]
    genes = conn.shape[1]
    return pl.pallas_call(
        functools.partial(hist_kernel, scale),
        out_shape=(
            pltpu.VMEM((powers, genes), jnp.float32),
            pltpu.VMEM((powers, BINS), jnp.float32),
        ),
        in_specs=[SMEM, SMEM, VMEM, VMEM],
        out_specs=(VMEM, VMEM),
        scratch_shapes=[pltpu.VMEM(conn.shape, jnp.float32)] * 2,
        compiler_params=PARAMS,
        name="histogram",
    )(power_order, slot, in_vmem(conn), in_vmem(other))


def fit_kernel(log_total, hist_ref, other_ref, fit_ref, slope_ref):
    hist = hist_ref[...] + other_ref[...]
    powers = hist.shape[0]
    lane = lax.broadcasted_iota(jnp.int32, (powers, BINS), 1)
    centers = lane.astype(jnp.float32) * (log_total / (BINS - 1))

    def total(x):
        return jnp.sum(x, axis=1, keepdims=True)

    weight_sum = total(hist)
    ylog = jnp.log(hist + 1.0) - log_total
    xdev = centers - total(hist * centers) / weight_sum
    ydev = ylog - total(hist * ylog) / weight_sum
    sxx = jnp.maximum(total(hist * xdev * xdev) / weight_sum, 0.05)
    syy = jnp.maximum(total(hist * ydev * ydev) / weight_sum, 0.05)
    sxy = total(hist * xdev * ydev) / weight_sum
    own = lax.broadcasted_iota(jnp.int32, (powers, BINS), 0) == lane

    def store(ref, column):
        ref[...] = jnp.sum(jnp.where(own, column, 0.0), axis=0)[:powers]

    store(fit_ref, -sxy * jnp.abs(sxy) / (sxx * syy))
    store(slope_ref, sxy / sxx)


def scale_free_fit(hist, other, log_total):
    powers = hist.shape[0]
    return pl.pallas_call(
        functools.partial(fit_kernel, log_total),
        out_shape=(jax.ShapeDtypeStruct((powers,), jnp.float32),) * 2,
        in_specs=[VMEM, VMEM],
        out_specs=(VMEM, VMEM),
        compiler_params=PARAMS,
        name="scale_free_fit",
    )(in_vmem(hist), in_vmem(other))


def on_device(expression, power_order):
    rows, cols = lax.axis_size("row"), lax.axis_size("col")
    count = rows * cols
    powers = power_order.shape[0]
    log_total = math.log(expression.shape[0] * count)
    panel_masks, partner_masks = plan(rows, cols)
    far, core = panel_masks[0], partner_masks[-1]
    low, sides = partner_masks[0], partner_masks[1:-1]

    partner = spread(expression, partner_masks, count)
    panel = spread(expression, panel_masks, count)
    keys = list(panel)
    front = [k for k in keys if not k & far & ~core] + [far]
    rear = [k for k in keys if k not in front]

    index = lax.axis_index(AXES)
    slot = sum(((index // (mask & ~core)) % 2) << i for i, mask in enumerate(panel_masks))
    slot = jnp.reshape(slot, (1,)).astype(jnp.int32)

    relayed = [k for k in partner if bin(k & ~core).count("1") > 1]
    waves = [
        ([0], [0]),
        (front, [core] + sides),
        (front[1:], [0]),
        (front, [k ^ core for k in sides] + [low, low ^ core]),
        (front, [k for k in relayed if not k & core]),
        (front, [k for k in relayed if k & core]),
    ]
    done = []
    parts = {k: [] for k in keys}
    for n, (panels, partners) in enumerate(waves):
        done.append(power_sums([panel[k] for k in panels], [partner[k] for k in partners], powers))
        for i, k in enumerate(panels):
            parts[k].append((n, i))
    everyone = list(partner)
    early, late = everyone[CHUNK:], everyone[:CHUNK]
    if early:
        done.append(power_sums([panel[k] for k in rear], [partner[k] for k in early], powers))
    for i, k in enumerate(rear):
        parts[k] += [(len(done) - 1, i)] * bool(early) + [(None, i)]
    conn = last_sums(
        slot,
        [panel[k] for k in rear],
        [partner[k] for k in late],
        done,
        [parts[k] for k in keys],
        powers,
    )

    for mask in panel_masks[:0:-1]:
        conn = conn + swap(conn, mask, count)
    log_conn, hist = histogram(
        power_order, slot, conn, swap(conn, far, count), (BINS - 1) / log_total
    )
    for mask in partner_masks[:-1]:
        hist = hist + swap(hist, (mask & ~core) ^ core, count)
    fit, slope = scale_free_fit(hist, swap(hist, core, count), log_total)
    return (log_conn.T, fit, slope)


def solution(mesh):
    placed = (P(AXES, None), P())
    return jax.shard_map(
        on_device,
        mesh=mesh,
        in_specs=placed,
        out_specs=(P(AXES, None), P(), P()),
        check_vma=False,
    )
```

```python
import functools
import math

import jax
import jax.numpy as jnp
from jax import lax
from jax.experimental import pallas as pl
from jax.experimental.pallas import tpu as pltpu
from jax.sharding import PartitionSpec as P


AXES = ("row", "col")
BINS = 128
CHUNK = 8
VMEM = pl.BlockSpec(memory_space=pltpu.VMEM)
SMEM = pl.BlockSpec(memory_space=pltpu.SMEM)
PARAMS = pltpu.CompilerParams(vmem_limit_bytes=16 * 2**20)


def swap(x, mask, count):
    return lax.ppermute(x, AXES, [(i, i ^ mask) for i in range(count)])


def spread(block, masks, count):
    held = {0: block}
    for mask in masks:
        for key in list(held):
            held[key ^ mask] = swap(held[key], mask, count)
    return held


def plan(rows, cols):
    row_masks = [cols << i for i in range(rows.bit_length() - 1)]
    core, *col_masks = [1 << i for i in range(cols.bit_length() - 1)]
    panel_masks = [row_masks[-1]] + col_masks
    partner_masks = row_masks[-2::-1] + [core]
    return panel_masks, partner_masks


def in_vmem(x):
    return pltpu.with_memory_space_constraint(x, pltpu.VMEM)


def pair_sum(values):
    while len(values) > 1:
        values = [a + b for a, b in zip(values[::2], values[1::2])]
    return values[0]


def joined(refs):
    return refs[0][...] if len(refs) == 1 else jnp.concatenate([r[...] for r in refs], axis=0)


def add_powers(panel_refs, partner_refs, total_ref):
    genes, samples = panel_refs[0].shape
    powers = total_ref.shape[1]
    panel = joined(panel_refs)
    many = len(panel_refs) > 1
    groups = [partner_refs] if many else [[ref] for ref in partner_refs]
    begun = False
    for group in groups:
        corr = lax.dot_general(
            joined(group), panel, (((1,), (1,)), ((), ())), preferred_element_type=jnp.float32
        )
        for low in range(0, corr.shape[0], genes):
            for i in range(len(panel_refs)):
                block = corr[low : low + genes, i * genes : (i + 1) * genes]
                magnitude = jnp.abs(block * (1.0 / samples))
                square = magnitude * magnitude
                current = [magnitude, square]
                for power in range(powers):
                    part = jnp.sum(current[power % 2].reshape(-1, 8, genes), axis=0)
                    total_ref[i, power] = total_ref[i, power] + part if begun else part
                    if power + 2 < powers:
                        current[power % 2] = current[power % 2] * square
            begun = True


def power_kernel(n_panel, *refs):
    out_ref, total_ref = refs[-2:]
    add_powers(refs[:n_panel], refs[n_panel:-2], total_ref)
    for i in range(n_panel):
        out_ref[i] = jnp.sum(total_ref[i], axis=1)


def power_sums(panels, partners, powers):
    genes, samples = panels[0].shape
    outs = []
    for first in range(0, len(partners), CHUNK):
        some = partners[first : first + CHUNK]
        flops = len(panels) * len(some) * genes * genes * 2 * samples
        outs.append(
            pl.pallas_call(
                functools.partial(power_kernel, len(panels)),
                out_shape=jax.ShapeDtypeStruct((len(panels), powers, genes), jnp.float32),
                in_specs=[VMEM] * (len(panels) + len(some)),
                out_specs=VMEM,
                scratch_shapes=[pltpu.VMEM((len(panels), powers, 8, genes), jnp.float32)],
                compiler_params=PARAMS,
                cost_estimate=pl.CostEstimate(flops=flops, bytes_accessed=0, transcendentals=0),
                name="power_sums",
            )(*map(in_vmem, panels), *map(in_vmem, some))
        )
    return functools.reduce(jnp.add, outs)


def own_slot(panel_bits):
    index = lax.axis_index("row") * lax.axis_size("col") + lax.axis_index("col")
    return sum(((index // bit) % 2) << i for i, bit in enumerate(panel_bits))


def last_kernel(panel_bits, n_panel, n_partner, parts, order_hbm, *refs):
    part_refs = refs[n_panel + n_partner : -5]
    conn_ref, total_ref, natural, order, arrived = refs[-5:]
    slots = len(parts)
    powers = total_ref.shape[1]
    fetch = pltpu.make_async_copy(order_hbm, order, arrived)
    fetch.start()
    mine = own_slot(panel_bits)
    add_powers(refs[:n_panel], refs[n_panel : n_panel + n_partner], total_ref)
    for i, where in enumerate(parts):
        values = [part_refs[a][b] for a, b in where if a is not None]
        values += [jnp.sum(total_ref[b], axis=1) for a, b in where if a is None]
        natural[i] = functools.reduce(jnp.add, values)
    fetch.wait()
    for t in range(powers):
        at = order[t]
        for i in range(slots):
            slot = jnp.bitwise_xor(mine, i)
            conn_ref[pl.ds(t * slots + slot, 1), :] = natural[i, pl.ds(at, 1), :]


def last_sums(panel_bits, power_order, panels, partners, done, parts):
    genes, samples = panels[0].shape
    powers = power_order.shape[0]
    flops = len(panels) * len(partners) * genes * genes * 2 * samples
    return pl.pallas_call(
        functools.partial(last_kernel, panel_bits, len(panels), len(partners), parts),
        out_shape=jax.ShapeDtypeStruct((powers * len(parts), genes), jnp.float32),
        in_specs=[pl.BlockSpec(memory_space=pltpu.HBM)]
        + [VMEM] * (len(panels) + len(partners) + len(done)),
        out_specs=VMEM,
        scratch_shapes=[
            pltpu.VMEM((len(panels), powers, 8, genes), jnp.float32),
            pltpu.VMEM((len(parts), powers, genes), jnp.float32),
            pltpu.SMEM((powers,), jnp.int32),
            pltpu.SemaphoreType.DMA(()),
        ],
        compiler_params=PARAMS,
        cost_estimate=pl.CostEstimate(flops=flops, bytes_accessed=0, transcendentals=0),
        name="last_sums",
    )(power_order, *map(in_vmem, panels), *map(in_vmem, partners), *map(in_vmem, done))


def hist_kernel(scale, panel_bits, conn_ref, other_ref, log_ref, hist_ref, logs, places):
    rows, genes = conn_ref.shape
    powers = log_ref.shape[0]
    slots = rows // powers
    mine = own_slot(panel_bits)
    logs[...] = jnp.log(conn_ref[...] + other_ref[...])
    places[...] = logs[...] * scale
    levels = lax.broadcasted_iota(jnp.int32, (BINS, genes), 0).astype(jnp.float32)
    lane = lax.broadcasted_iota(jnp.int32, (BINS, BINS), 1)
    table = jnp.zeros((BINS, BINS), jnp.float32)
    for t in range(powers):
        first = t * slots
        log_ref[pl.ds(t, 1), :] = logs[pl.ds(first + mine, 1), :]
        away = pair_sum(
            [
                jnp.minimum(jnp.abs(places[pl.ds(first + m, 1), :] - levels), 1.0)
                for m in range(slots)
            ]
        )
        table = jnp.where(lane == t, jnp.sum(slots - away, axis=1, keepdims=True), table)
    hist_ref[...] = table.T[:powers]


def histogram(panel_bits, powers, conn, other, scale):
    genes = conn.shape[1]
    return pl.pallas_call(
        functools.partial(hist_kernel, scale, panel_bits),
        out_shape=(
            pltpu.VMEM((powers, genes), jnp.float32),
            pltpu.VMEM((powers, BINS), jnp.float32),
        ),
        in_specs=[VMEM, VMEM],
        out_specs=(VMEM, VMEM),
        scratch_shapes=[pltpu.VMEM(conn.shape, jnp.float32)] * 2,
        compiler_params=PARAMS,
        name="histogram",
    )(in_vmem(conn), in_vmem(other))


def fit_kernel(log_total, hist_ref, other_ref, fit_ref, slope_ref):
    hist = hist_ref[...] + other_ref[...]
    powers = hist.shape[0]
    lane = lax.broadcasted_iota(jnp.int32, (powers, BINS), 1)
    centers = lane.astype(jnp.float32) * (log_total / (BINS - 1))

    def total(x):
        return jnp.sum(x, axis=1, keepdims=True)

    weight_sum = total(hist)
    ylog = jnp.log(hist + 1.0) - log_total
    xdev = centers - total(hist * centers) / weight_sum
    ydev = ylog - total(hist * ylog) / weight_sum
    sxx = jnp.maximum(total(hist * xdev * xdev) / weight_sum, 0.05)
    syy = jnp.maximum(total(hist * ydev * ydev) / weight_sum, 0.05)
    sxy = total(hist * xdev * ydev) / weight_sum
    own = lax.broadcasted_iota(jnp.int32, (powers, BINS), 0) == lane

    def store(ref, column):
        ref[...] = jnp.sum(jnp.where(own, column, 0.0), axis=0)[:powers]

    store(fit_ref, -sxy * jnp.abs(sxy) / (sxx * syy))
    store(slope_ref, sxy / sxx)


def scale_free_fit(hist, other, log_total):
    powers = hist.shape[0]
    return pl.pallas_call(
        functools.partial(fit_kernel, log_total),
        out_shape=(jax.ShapeDtypeStruct((powers,), jnp.float32),) * 2,
        in_specs=[VMEM, VMEM],
        out_specs=(VMEM, VMEM),
        compiler_params=PARAMS,
        name="scale_free_fit",
    )(in_vmem(hist), in_vmem(other))


def on_device(expression, power_order):
    rows, cols = lax.axis_size("row"), lax.axis_size("col")
    count = rows * cols
    powers = power_order.shape[0]
    log_total = math.log(expression.shape[0] * count)
    panel_masks, partner_masks = plan(rows, cols)
    far, core = panel_masks[0], partner_masks[-1]
    low, sides = partner_masks[0], partner_masks[1:-1]

    partner = spread(expression, partner_masks, count)
    panel = spread(expression, panel_masks, count)
    keys = list(panel)
    front = [k for k in keys if not k & far & ~core] + [far]
    rear = [k for k in keys if k not in front]

    panel_bits = [mask & ~core for mask in panel_masks]

    relayed = [k for k in partner if bin(k & ~core).count("1") > 1]
    waves = [
        ([0], [0]),
        (front, [core] + sides),
        (front[1:], [0]),
        (front, [k ^ core for k in sides] + [low, low ^ core]),
        (front, [k for k in relayed if not k & core]),
        (front, [k for k in relayed if k & core]),
    ]
    done = []
    parts = {k: [] for k in keys}
    for n, (panels, partners) in enumerate(waves):
        done.append(power_sums([panel[k] for k in panels], [partner[k] for k in partners], powers))
        for i, k in enumerate(panels):
            parts[k].append((n, i))
    everyone = list(partner)
    early, late = everyone[CHUNK:], everyone[:CHUNK]
    if early:
        done.append(power_sums([panel[k] for k in rear], [partner[k] for k in early], powers))
    for i, k in enumerate(rear):
        parts[k] += [(len(done) - 1, i)] * bool(early) + [(None, i)]
    conn = last_sums(
        panel_bits,
        power_order,
        [panel[k] for k in rear],
        [partner[k] for k in late],
        done,
        [parts[k] for k in keys],
    )

    for mask in panel_masks[:0:-1]:
        conn = conn + swap(conn, mask, count)
    log_conn, hist = histogram(
        panel_bits, powers, conn, swap(conn, far, count), (BINS - 1) / log_total
    )
    for mask in partner_masks[:-1]:
        hist = hist + swap(hist, (mask & ~core) ^ core, count)
    fit, slope = scale_free_fit(hist, swap(hist, core, count), log_total)
    return (log_conn.T, fit, slope)


def solution(mesh):
    placed = (P(AXES, None), P())
    return jax.shard_map(
        on_device,
        mesh=mesh,
        in_specs=placed,
        out_specs=(P(AXES, None), P(), P()),
        check_vma=False,
    )
```

```python
import functools
import math

import jax
import jax.numpy as jnp
from jax import lax
from jax.experimental import pallas as pl
from jax.experimental.pallas import tpu as pltpu
from jax.sharding import PartitionSpec as P


AXES = ("row", "col")
BINS = 128
CHUNK = 8
VMEM = pl.BlockSpec(memory_space=pltpu.VMEM)
SMEM = pl.BlockSpec(memory_space=pltpu.SMEM)
PARAMS = pltpu.CompilerParams(vmem_limit_bytes=16 * 2**20)


def swap(x, mask, count):
    return lax.ppermute(x, AXES, [(i, i ^ mask) for i in range(count)])


def spread(block, masks, count):
    held = {0: block}
    for mask in masks:
        for key in list(held):
            held[key ^ mask] = swap(held[key], mask, count)
    return held


def plan(rows, cols):
    row_masks = [cols << i for i in range(rows.bit_length() - 1)]
    core, *col_masks = [1 << i for i in range(cols.bit_length() - 1)]
    panel_masks = [row_masks[-1]] + col_masks
    partner_masks = row_masks[-2::-1] + [core]
    return panel_masks, partner_masks


def in_vmem(x):
    return pltpu.with_memory_space_constraint(x, pltpu.VMEM)


def pair_sum(values):
    while len(values) > 1:
        values = [a + b for a, b in zip(values[::2], values[1::2])]
    return values[0]


def joined(refs):
    return refs[0][...] if len(refs) == 1 else jnp.concatenate([r[...] for r in refs], axis=0)


def add_powers(panel_refs, partner_refs, total_ref):
    genes, samples = panel_refs[0].shape
    powers = total_ref.shape[1]
    panel = joined(panel_refs)
    many = len(panel_refs) > 1
    groups = [partner_refs] if many else [[ref] for ref in partner_refs]
    begun = False
    for group in groups:
        corr = lax.dot_general(
            joined(group), panel, (((1,), (1,)), ((), ())), preferred_element_type=jnp.float32
        )
        for low in range(0, corr.shape[0], genes):
            for i in range(len(panel_refs)):
                block = corr[low : low + genes, i * genes : (i + 1) * genes]
                magnitude = jnp.abs(block * (1.0 / samples))
                square = magnitude * magnitude
                current = [magnitude, square]
                for power in range(powers):
                    part = jnp.sum(current[power % 2].reshape(-1, 8, genes), axis=0)
                    total_ref[i, power] = total_ref[i, power] + part if begun else part
                    if power + 2 < powers:
                        current[power % 2] = current[power % 2] * square
            begun = True


def power_kernel(n_panel, *refs):
    out_ref, total_ref = refs[-2:]
    add_powers(refs[:n_panel], refs[n_panel:-2], total_ref)
    for i in range(n_panel):
        out_ref[i] = jnp.sum(total_ref[i], axis=1)


def power_sums(panels, partners, powers):
    genes, samples = panels[0].shape
    outs = []
    for first in range(0, len(partners), CHUNK):
        some = partners[first : first + CHUNK]
        flops = len(panels) * len(some) * genes * genes * 2 * samples
        outs.append(
            pl.pallas_call(
                functools.partial(power_kernel, len(panels)),
                out_shape=jax.ShapeDtypeStruct((len(panels), powers, genes), jnp.float32),
                in_specs=[VMEM] * (len(panels) + len(some)),
                out_specs=VMEM,
                scratch_shapes=[pltpu.VMEM((len(panels), powers, 8, genes), jnp.float32)],
                compiler_params=PARAMS,
                cost_estimate=pl.CostEstimate(flops=flops, bytes_accessed=0, transcendentals=0),
                name="power_sums",
            )(*map(in_vmem, panels), *map(in_vmem, some))
        )
    return functools.reduce(jnp.add, outs)


def own_slot(panel_bits):
    index = lax.axis_index("row") * lax.axis_size("col") + lax.axis_index("col")
    return sum(((index // bit) % 2) << i for i, bit in enumerate(panel_bits))


def last_kernel(panel_bits, n_panel, n_partner, parts, order_hbm, *refs):
    part_refs = refs[n_panel + n_partner : -6]
    conn_ref, total_ref, natural, packed, order, arrived = refs[-6:]
    slots = len(parts)
    powers = total_ref.shape[1]
    fetch = pltpu.make_async_copy(order_hbm, order, arrived)
    fetch.start()
    mine = own_slot(panel_bits)
    add_powers(refs[:n_panel], refs[n_panel : n_panel + n_partner], total_ref)
    for i, where in enumerate(parts):
        values = [part_refs[a][b] for a, b in where if a is not None]
        values += [jnp.sum(total_ref[b], axis=1) for a, b in where if a is None]
        natural[i] = functools.reduce(jnp.add, values) - (0.0 if i else 1.0)
    fetch.wait()
    for t in range(powers):
        at = order[t]
        for i in range(slots):
            slot = jnp.bitwise_xor(mine, i)
            packed[pl.ds(t * slots + slot, 1), :] = natural[i, pl.ds(at, 1), :]
    conn_ref[...] = packed[...].astype(conn_ref.dtype)


def last_sums(panel_bits, power_order, panels, partners, done, parts):
    genes, samples = panels[0].shape
    powers = power_order.shape[0]
    flops = len(panels) * len(partners) * genes * genes * 2 * samples
    return pl.pallas_call(
        functools.partial(last_kernel, panel_bits, len(panels), len(partners), parts),
        out_shape=jax.ShapeDtypeStruct((powers * len(parts), genes), jnp.bfloat16),
        in_specs=[pl.BlockSpec(memory_space=pltpu.HBM)]
        + [VMEM] * (len(panels) + len(partners) + len(done)),
        out_specs=VMEM,
        scratch_shapes=[
            pltpu.VMEM((len(panels), powers, 8, genes), jnp.float32),
            pltpu.VMEM((len(parts), powers, genes), jnp.float32),
            pltpu.VMEM((powers * len(parts), genes), jnp.float32),
            pltpu.SMEM((powers,), jnp.int32),
            pltpu.SemaphoreType.DMA(()),
        ],
        compiler_params=PARAMS,
        cost_estimate=pl.CostEstimate(flops=flops, bytes_accessed=0, transcendentals=0),
        name="last_sums",
    )(power_order, *map(in_vmem, panels), *map(in_vmem, partners), *map(in_vmem, done))


def hist_kernel(scale, panel_bits, conn_ref, other_ref, log_ref, hist_ref, logs, places):
    rows, genes = conn_ref.shape
    powers = log_ref.shape[0]
    slots = rows // powers
    mine = own_slot(panel_bits)
    less = conn_ref[...].astype(jnp.float32) + other_ref[...].astype(jnp.float32)
    logs[...] = jnp.log(less + 1.0)
    places[...] = logs[...] * scale
    levels = lax.broadcasted_iota(jnp.int32, (BINS, genes), 0).astype(jnp.float32)
    lane = lax.broadcasted_iota(jnp.int32, (BINS, BINS), 1)
    table = jnp.zeros((BINS, BINS), jnp.float32)
    for t in range(powers):
        first = t * slots
        log_ref[pl.ds(t, 1), :] = logs[pl.ds(first + mine, 1), :]
        away = pair_sum(
            [
                jnp.minimum(jnp.abs(places[pl.ds(first + m, 1), :] - levels), 1.0)
                for m in range(slots)
            ]
        )
        table = jnp.where(lane == t, jnp.sum(slots - away, axis=1, keepdims=True), table)
    hist_ref[...] = table.T[:powers]


def histogram(panel_bits, powers, conn, other, scale):
    genes = conn.shape[1]
    return pl.pallas_call(
        functools.partial(hist_kernel, scale, panel_bits),
        out_shape=(
            pltpu.VMEM((powers, genes), jnp.float32),
            pltpu.VMEM((powers, BINS), jnp.float32),
        ),
        in_specs=[VMEM, VMEM],
        out_specs=(VMEM, VMEM),
        scratch_shapes=[pltpu.VMEM(conn.shape, jnp.float32)] * 2,
        compiler_params=PARAMS,
        name="histogram",
    )(in_vmem(conn), in_vmem(other))


def fit_kernel(log_total, hist_ref, other_ref, fit_ref, slope_ref):
    hist = hist_ref[...] + other_ref[...]
    powers = hist.shape[0]
    lane = lax.broadcasted_iota(jnp.int32, (powers, BINS), 1)
    centers = lane.astype(jnp.float32) * (log_total / (BINS - 1))

    def total(x):
        return jnp.sum(x, axis=1, keepdims=True)

    weight_sum = total(hist)
    ylog = jnp.log(hist + 1.0) - log_total
    xdev = centers - total(hist * centers) / weight_sum
    ydev = ylog - total(hist * ylog) / weight_sum
    sxx = jnp.maximum(total(hist * xdev * xdev) / weight_sum, 0.05)
    syy = jnp.maximum(total(hist * ydev * ydev) / weight_sum, 0.05)
    sxy = total(hist * xdev * ydev) / weight_sum
    own = lax.broadcasted_iota(jnp.int32, (powers, BINS), 0) == lane

    def store(ref, column):
        ref[...] = jnp.sum(jnp.where(own, column, 0.0), axis=0)[:powers]

    store(fit_ref, -sxy * jnp.abs(sxy) / (sxx * syy))
    store(slope_ref, sxy / sxx)


def scale_free_fit(hist, other, log_total):
    powers = hist.shape[0]
    return pl.pallas_call(
        functools.partial(fit_kernel, log_total),
        out_shape=(jax.ShapeDtypeStruct((powers,), jnp.float32),) * 2,
        in_specs=[VMEM, VMEM],
        out_specs=(VMEM, VMEM),
        compiler_params=PARAMS,
        name="scale_free_fit",
    )(in_vmem(hist), in_vmem(other))


def on_device(expression, power_order):
    rows, cols = lax.axis_size("row"), lax.axis_size("col")
    count = rows * cols
    powers = power_order.shape[0]
    log_total = math.log(expression.shape[0] * count)
    panel_masks, partner_masks = plan(rows, cols)
    far, core = panel_masks[0], partner_masks[-1]
    low, sides = partner_masks[0], partner_masks[1:-1]

    partner = spread(expression, partner_masks, count)
    panel = spread(expression, panel_masks, count)
    keys = list(panel)
    front = [k for k in keys if not k & far & ~core] + [far]
    rear = [k for k in keys if k not in front]

    panel_bits = [mask & ~core for mask in panel_masks]

    relayed = [k for k in partner if bin(k & ~core).count("1") > 1]
    waves = [
        ([0], [0]),
        (front, [core] + sides),
        (front[1:], [0]),
        (front, [k ^ core for k in sides] + [low, low ^ core]),
        (front, [k for k in relayed if not k & core]),
        (front, [k for k in relayed if k & core]),
    ]
    done = []
    parts = {k: [] for k in keys}
    for n, (panels, partners) in enumerate(waves):
        done.append(power_sums([panel[k] for k in panels], [partner[k] for k in partners], powers))
        for i, k in enumerate(panels):
            parts[k].append((n, i))
    everyone = list(partner)
    early, late = everyone[CHUNK:], everyone[:CHUNK]
    if early:
        done.append(power_sums([panel[k] for k in rear], [partner[k] for k in early], powers))
    for i, k in enumerate(rear):
        parts[k] += [(len(done) - 1, i)] * bool(early) + [(None, i)]
    conn = last_sums(
        panel_bits,
        power_order,
        [panel[k] for k in rear],
        [partner[k] for k in late],
        done,
        [parts[k] for k in keys],
    )

    for mask in panel_masks[:0:-1]:
        other = swap(conn, mask, count)
        conn = (conn.astype(jnp.float32) + other.astype(jnp.float32)).astype(conn.dtype)
    log_conn, hist = histogram(
        panel_bits, powers, conn, swap(conn, far, count), (BINS - 1) / log_total
    )
    for mask in partner_masks[:-1]:
        hist = hist + swap(hist, (mask & ~core) ^ core, count)
    fit, slope = scale_free_fit(hist, swap(hist, core, count), log_total)
    return (log_conn.T, fit, slope)


def solution(mesh):
    placed = (P(AXES, None), P())
    return jax.shard_map(
        on_device,
        mesh=mesh,
        in_specs=placed,
        out_specs=(P(AXES, None), P(), P()),
        check_vma=False,
    )
```

```python
import functools
import math

import jax
import jax.numpy as jnp
from jax import lax
from jax.experimental import pallas as pl
from jax.experimental.pallas import tpu as pltpu
from jax.sharding import PartitionSpec as P


AXES = ("row", "col")
BINS = 128
CHUNK = 8
FRONT, REAR = -1, -2
VMEM = pl.BlockSpec(memory_space=pltpu.VMEM)
SMEM = pl.BlockSpec(memory_space=pltpu.SMEM)
PARAMS = pltpu.CompilerParams(vmem_limit_bytes=16 * 2**20)


def swap(x, mask, count):
    return lax.ppermute(x, AXES, [(i, i ^ mask) for i in range(count)])


def spread(block, masks, count):
    held = {0: block}
    for mask in masks:
        for key in list(held):
            held[key ^ mask] = swap(held[key], mask, count)
    return held


def plan(rows, cols):
    row_masks = [cols << i for i in range(rows.bit_length() - 1)]
    core, *col_masks = [1 << i for i in range(cols.bit_length() - 1)]
    panel_masks = [row_masks[-1]] + col_masks
    partner_masks = row_masks[-2::-1] + [core]
    return panel_masks, partner_masks


def in_vmem(x):
    return pltpu.with_memory_space_constraint(x, pltpu.VMEM)


def pair_sum(values):
    while len(values) > 1:
        values = [a + b for a, b in zip(values[::2], values[1::2])]
    return values[0]


def joined(refs):
    return refs[0][...] if len(refs) == 1 else jnp.concatenate([r[...] for r in refs], axis=0)


def add_powers(panel_refs, partner_refs, total_ref):
    genes, samples = panel_refs[0].shape
    powers = total_ref.shape[1]
    panel = joined(panel_refs)
    many = len(panel_refs) > 1
    groups = [partner_refs] if many else [[ref] for ref in partner_refs]
    begun = False
    for group in groups:
        corr = lax.dot_general(
            joined(group), panel, (((1,), (1,)), ((), ())), preferred_element_type=jnp.float32
        )
        for low in range(0, corr.shape[0], genes):
            for i in range(len(panel_refs)):
                block = corr[low : low + genes, i * genes : (i + 1) * genes]
                magnitude = jnp.abs(block * (1.0 / samples))
                square = magnitude * magnitude
                current = [magnitude, square]
                for power in range(powers):
                    part = jnp.sum(current[power % 2].reshape(-1, 8, genes), axis=0)
                    total_ref[i, power] = total_ref[i, power] + part if begun else part
                    if power + 2 < powers:
                        current[power % 2] = current[power % 2] * square
            begun = True


def power_kernel(n_panel, *refs):
    out_ref, total_ref = refs[-2:]
    add_powers(refs[:n_panel], refs[n_panel:-2], total_ref)
    for i in range(n_panel):
        out_ref[i] = jnp.sum(total_ref[i], axis=1)


def power_sums(panels, partners, powers):
    genes, samples = panels[0].shape
    outs = []
    for first in range(0, len(partners), CHUNK):
        some = partners[first : first + CHUNK]
        flops = len(panels) * len(some) * genes * genes * 2 * samples
        outs.append(
            pl.pallas_call(
                functools.partial(power_kernel, len(panels)),
                out_shape=jax.ShapeDtypeStruct((len(panels), powers, genes), jnp.float32),
                in_specs=[VMEM] * (len(panels) + len(some)),
                out_specs=VMEM,
                scratch_shapes=[pltpu.VMEM((len(panels), powers, 8, genes), jnp.float32)],
                compiler_params=PARAMS,
                cost_estimate=pl.CostEstimate(flops=flops, bytes_accessed=0, transcendentals=0),
                name="power_sums",
            )(*map(in_vmem, panels), *map(in_vmem, some))
        )
    return functools.reduce(jnp.add, outs)


def own_slot(panel_bits):
    index = lax.axis_index("row") * lax.axis_size("col") + lax.axis_index("col")
    return sum(((index // bit) % 2) << i for i, bit in enumerate(panel_bits))


def last_kernel(panel_bits, n_front, n_panel, n_partner, parts, order_hbm, *refs):
    front_refs, tail_ref, refs = refs[:n_front], refs[n_front], refs[n_front + 1 :]
    part_refs = refs[n_panel + n_partner : -6]
    conn_ref, front_total, total_ref, natural, order, arrived = refs[-6:]
    slots = len(parts)
    powers = total_ref.shape[1]
    fetch = pltpu.make_async_copy(order_hbm, order, arrived)
    fetch.start()
    mine = own_slot(panel_bits)
    add_powers(front_refs, [tail_ref], front_total)
    add_powers(refs[:n_panel], refs[n_panel : n_panel + n_partner], total_ref)
    for i, where in enumerate(parts):
        values = [part_refs[a][b] for a, b in where if a >= 0]
        values += [jnp.sum(front_total[b], axis=1) for a, b in where if a == FRONT]
        values += [jnp.sum(total_ref[b], axis=1) for a, b in where if a == REAR]
        natural[i] = functools.reduce(jnp.add, values)
    fetch.wait()
    for t in range(powers):
        at = order[t]
        for i in range(slots):
            slot = jnp.bitwise_xor(mine, i)
            conn_ref[pl.ds(t * slots + slot, 1), :] = natural[i, pl.ds(at, 1), :]


def last_sums(panel_bits, power_order, front, tail, panels, partners, done, parts):
    genes, samples = panels[0].shape
    powers = power_order.shape[0]
    flops = len(panels) * len(partners) * genes * genes * 2 * samples
    return pl.pallas_call(
        functools.partial(
            last_kernel, panel_bits, len(front), len(panels), len(partners), parts
        ),
        out_shape=jax.ShapeDtypeStruct((powers * len(parts), genes), jnp.float32),
        in_specs=[pl.BlockSpec(memory_space=pltpu.HBM)]
        + [VMEM] * (len(front) + 1 + len(panels) + len(partners) + len(done)),
        out_specs=VMEM,
        scratch_shapes=[
            pltpu.VMEM((len(front), powers, 8, genes), jnp.float32),
            pltpu.VMEM((len(panels), powers, 8, genes), jnp.float32),
            pltpu.VMEM((len(parts), powers, genes), jnp.float32),
            pltpu.SMEM((powers,), jnp.int32),
            pltpu.SemaphoreType.DMA(()),
        ],
        compiler_params=PARAMS,
        cost_estimate=pl.CostEstimate(flops=flops, bytes_accessed=0, transcendentals=0),
        name="last_sums",
    )(power_order, *map(in_vmem, [*front, tail, *panels, *partners, *done]))


def hist_kernel(scale, panel_bits, conn_ref, other_ref, log_ref, hist_ref, logs, places):
    rows, genes = conn_ref.shape
    powers = log_ref.shape[0]
    slots = rows // powers
    mine = own_slot(panel_bits)
    logs[...] = jnp.log(conn_ref[...] + other_ref[...])
    places[...] = logs[...] * scale
    levels = lax.broadcasted_iota(jnp.int32, (BINS, genes), 0).astype(jnp.float32)
    lane = lax.broadcasted_iota(jnp.int32, (BINS, BINS), 1)
    table = jnp.zeros((BINS, BINS), jnp.float32)
    for t in range(powers):
        first = t * slots
        log_ref[pl.ds(t, 1), :] = logs[pl.ds(first + mine, 1), :]
        away = pair_sum(
            [
                jnp.minimum(jnp.abs(places[pl.ds(first + m, 1), :] - levels), 1.0)
                for m in range(slots)
            ]
        )
        table = jnp.where(lane == t, jnp.sum(slots - away, axis=1, keepdims=True), table)
    hist_ref[...] = table.T[:powers]


def histogram(panel_bits, powers, conn, other, scale):
    genes = conn.shape[1]
    return pl.pallas_call(
        functools.partial(hist_kernel, scale, panel_bits),
        out_shape=(
            pltpu.VMEM((powers, genes), jnp.float32),
            pltpu.VMEM((powers, BINS), jnp.float32),
        ),
        in_specs=[VMEM, VMEM],
        out_specs=(VMEM, VMEM),
        scratch_shapes=[pltpu.VMEM(conn.shape, jnp.float32)] * 2,
        compiler_params=PARAMS,
        name="histogram",
    )(in_vmem(conn), in_vmem(other))


def fit_kernel(log_total, hist_ref, other_ref, fit_ref, slope_ref):
    hist = hist_ref[...] + other_ref[...]
    powers = hist.shape[0]
    lane = lax.broadcasted_iota(jnp.int32, (powers, BINS), 1)
    centers = lane.astype(jnp.float32) * (log_total / (BINS - 1))

    def total(x):
        return jnp.sum(x, axis=1, keepdims=True)

    weight_sum = total(hist)
    ylog = jnp.log(hist + 1.0) - log_total
    xdev = centers - total(hist * centers) / weight_sum
    ydev = ylog - total(hist * ylog) / weight_sum
    sxx = jnp.maximum(total(hist * xdev * xdev) / weight_sum, 0.05)
    syy = jnp.maximum(total(hist * ydev * ydev) / weight_sum, 0.05)
    sxy = total(hist * xdev * ydev) / weight_sum
    own = lax.broadcasted_iota(jnp.int32, (powers, BINS), 0) == lane

    def store(ref, column):
        ref[...] = jnp.sum(jnp.where(own, column, 0.0), axis=0)[:powers]

    store(fit_ref, -sxy * jnp.abs(sxy) / (sxx * syy))
    store(slope_ref, sxy / sxx)


def scale_free_fit(hist, other, log_total):
    powers = hist.shape[0]
    return pl.pallas_call(
        functools.partial(fit_kernel, log_total),
        out_shape=(jax.ShapeDtypeStruct((powers,), jnp.float32),) * 2,
        in_specs=[VMEM, VMEM],
        out_specs=(VMEM, VMEM),
        compiler_params=PARAMS,
        name="scale_free_fit",
    )(in_vmem(hist), in_vmem(other))


def on_device(expression, power_order):
    rows, cols = lax.axis_size("row"), lax.axis_size("col")
    count = rows * cols
    powers = power_order.shape[0]
    log_total = math.log(expression.shape[0] * count)
    panel_masks, partner_masks = plan(rows, cols)
    far, core = panel_masks[0], partner_masks[-1]
    low, sides = partner_masks[0], partner_masks[1:-1]

    partner = spread(expression, partner_masks, count)
    panel = spread(expression, panel_masks, count)
    keys = list(panel)
    front = [k for k in keys if not k & far & ~core] + [far]
    rear = [k for k in keys if k not in front]

    panel_bits = [mask & ~core for mask in panel_masks]

    relayed = [k for k in partner if bin(k & ~core).count("1") > 1]
    waves = [
        ([0], [0]),
        (front, [core] + sides),
        (front[1:], [0]),
        (front, [k ^ core for k in sides] + [low, low ^ core]),
        (front, [k for k in relayed if not k & core]),
        (front, [k for k in relayed if k & core][:-1]),
    ]
    tail = [k for k in relayed if k & core][-1]
    done = []
    parts = {k: [] for k in keys}
    for n, (panels, partners) in enumerate(wave for wave in waves if wave[1]):
        done.append(power_sums([panel[k] for k in panels], [partner[k] for k in partners], powers))
        for i, k in enumerate(panels):
            parts[k].append((n, i))
    everyone = list(partner)
    early, late = everyone[CHUNK:], everyone[:CHUNK]
    if early:
        done.append(power_sums([panel[k] for k in rear], [partner[k] for k in early], powers))
    for i, k in enumerate(rear):
        parts[k] += [(len(done) - 1, i)] * bool(early) + [(REAR, i)]
    for i, k in enumerate(front):
        parts[k].append((FRONT, i))
    conn = last_sums(
        panel_bits,
        power_order,
        [panel[k] for k in front],
        partner[tail],
        [panel[k] for k in rear],
        [partner[k] for k in late],
        done,
        [parts[k] for k in keys],
    )

    for mask in panel_masks[:0:-1]:
        conn = conn + swap(conn, mask, count)
    log_conn, hist = histogram(
        panel_bits, powers, conn, swap(conn, far, count), (BINS - 1) / log_total
    )
    for mask in partner_masks[:-1]:
        hist = hist + swap(hist, (mask & ~core) ^ core, count)
    fit, slope = scale_free_fit(hist, swap(hist, core, count), log_total)
    return (log_conn.T, fit, slope)


def solution(mesh):
    placed = (P(AXES, None), P())
    return jax.shard_map(
        on_device,
        mesh=mesh,
        in_specs=placed,
        out_specs=(P(AXES, None), P(), P()),
        check_vma=False,
    )
```

```python
import functools
import math

import jax
import jax.numpy as jnp
from jax import lax
from jax.experimental import pallas as pl
from jax.experimental.pallas import tpu as pltpu
from jax.sharding import PartitionSpec as P


AXES = ("row", "col")
BINS = 128
CHUNK = 8
FRONT, REAR = -1, -2
VMEM = pl.BlockSpec(memory_space=pltpu.VMEM)
SMEM = pl.BlockSpec(memory_space=pltpu.SMEM)
PARAMS = pltpu.CompilerParams(vmem_limit_bytes=16 * 2**20)


def swap(x, mask, count):
    return lax.ppermute(x, AXES, [(i, i ^ mask) for i in range(count)])


def spread(block, masks, count):
    held = {0: block}
    for mask in masks:
        for key in list(held):
            held[key ^ mask] = swap(held[key], mask, count)
    return held


def plan(rows, cols):
    row_masks = [cols << i for i in range(rows.bit_length() - 1)]
    core, *col_masks = [1 << i for i in range(cols.bit_length() - 1)]
    panel_masks = [row_masks[-1]] + col_masks
    partner_masks = row_masks[-2::-1] + [core]
    return panel_masks, partner_masks


def in_vmem(x):
    return pltpu.with_memory_space_constraint(x, pltpu.VMEM)


def pair_sum(values):
    while len(values) > 1:
        values = [a + b for a, b in zip(values[::2], values[1::2])]
    return values[0]


def joined(refs):
    return refs[0][...] if len(refs) == 1 else jnp.concatenate([r[...] for r in refs], axis=0)


def add_powers(panel_refs, partner_refs, total_ref):
    genes, samples = panel_refs[0].shape
    powers = total_ref.shape[1]
    panel = joined(panel_refs)
    many = len(panel_refs) > 1
    groups = [partner_refs] if many else [[ref] for ref in partner_refs]
    begun = False
    for group in groups:
        corr = lax.dot_general(
            joined(group), panel, (((1,), (1,)), ((), ())), preferred_element_type=jnp.float32
        )
        for low in range(0, corr.shape[0], genes):
            for i in range(len(panel_refs)):
                block = corr[low : low + genes, i * genes : (i + 1) * genes]
                magnitude = jnp.abs(block * (1.0 / samples))
                square = magnitude * magnitude
                current = [magnitude, square]
                for power in range(powers):
                    part = jnp.sum(current[power % 2].reshape(-1, 8, genes), axis=0)
                    total_ref[i, power] = total_ref[i, power] + part if begun else part
                    if power + 2 < powers:
                        current[power % 2] = current[power % 2] * square
            begun = True


def power_kernel(n_panel, *refs):
    out_ref, total_ref = refs[-2:]
    add_powers(refs[:n_panel], refs[n_panel:-2], total_ref)
    for i in range(n_panel):
        out_ref[i] = jnp.sum(total_ref[i], axis=1)


def power_sums(panels, partners, powers):
    genes, samples = panels[0].shape
    outs = []
    for first in range(0, len(partners), CHUNK):
        some = partners[first : first + CHUNK]
        flops = len(panels) * len(some) * genes * genes * 2 * samples
        outs.append(
            pl.pallas_call(
                functools.partial(power_kernel, len(panels)),
                out_shape=jax.ShapeDtypeStruct((len(panels), powers, genes), jnp.float32),
                in_specs=[VMEM] * (len(panels) + len(some)),
                out_specs=VMEM,
                scratch_shapes=[pltpu.VMEM((len(panels), powers, 8, genes), jnp.float32)],
                compiler_params=PARAMS,
                cost_estimate=pl.CostEstimate(flops=flops, bytes_accessed=0, transcendentals=0),
                name="power_sums",
            )(*map(in_vmem, panels), *map(in_vmem, some))
        )
    return functools.reduce(jnp.add, outs)


def own_slot(panel_bits):
    index = lax.axis_index("row") * lax.axis_size("col") + lax.axis_index("col")
    return sum(((index // bit) % 2) << i for i, bit in enumerate(panel_bits))


def last_kernel(panel_bits, n_front, n_panel, n_partner, parts, order_hbm, *refs):
    front_refs, tail_ref, refs = refs[:n_front], refs[n_front], refs[n_front + 1 :]
    part_refs = refs[n_panel + n_partner : -6]
    conn_ref, front_total, total_ref, natural, order, arrived = refs[-6:]
    slots = len(parts)
    powers = total_ref.shape[1]
    fetch = pltpu.make_async_copy(order_hbm, order, arrived)
    fetch.start()
    mine = own_slot(panel_bits)
    add_powers(front_refs, [tail_ref], front_total)
    add_powers(refs[:n_panel], refs[n_panel : n_panel + n_partner], total_ref)
    for i, where in enumerate(parts):
        values = [part_refs[a][b] for a, b in where if a >= 0]
        values += [jnp.sum(front_total[b], axis=1) for a, b in where if a == FRONT]
        values += [jnp.sum(total_ref[b], axis=1) for a, b in where if a == REAR]
        natural[i] = functools.reduce(jnp.add, values)
    fetch.wait()
    for t in range(powers):
        at = order[t]
        for i in range(slots):
            slot = jnp.bitwise_xor(mine, i)
            conn_ref[pl.ds(t * slots + slot, 1), :] = natural[i, pl.ds(at, 1), :]


def last_sums(panel_bits, power_order, front, tail, panels, partners, done, parts):
    genes, samples = panels[0].shape
    powers = power_order.shape[0]
    flops = len(panels) * len(partners) * genes * genes * 2 * samples
    return pl.pallas_call(
        functools.partial(
            last_kernel, panel_bits, len(front), len(panels), len(partners), parts
        ),
        out_shape=jax.ShapeDtypeStruct((powers * len(parts), genes), jnp.float32),
        in_specs=[pl.BlockSpec(memory_space=pltpu.HBM)]
        + [VMEM] * (len(front) + 1 + len(panels) + len(partners) + len(done)),
        out_specs=VMEM,
        scratch_shapes=[
            pltpu.VMEM((len(front), powers, 8, genes), jnp.float32),
            pltpu.VMEM((len(panels), powers, 8, genes), jnp.float32),
            pltpu.VMEM((len(parts), powers, genes), jnp.float32),
            pltpu.SMEM((powers,), jnp.int32),
            pltpu.SemaphoreType.DMA(()),
        ],
        compiler_params=PARAMS,
        cost_estimate=pl.CostEstimate(flops=flops, bytes_accessed=0, transcendentals=0),
        name="last_sums",
    )(power_order, *map(in_vmem, [*front, tail, *panels, *partners, *done]))


def hist_kernel(scale, panel_bits, conn_ref, other_ref, log_ref, hist_ref, logs, places):
    rows, genes = conn_ref.shape
    powers = log_ref.shape[0]
    slots = rows // powers
    mine = own_slot(panel_bits)
    logs[...] = jnp.log(conn_ref[...] + other_ref[...])
    places[...] = logs[...] * scale
    levels = lax.broadcasted_iota(jnp.int32, (BINS, genes), 0).astype(jnp.float32)
    lane = lax.broadcasted_iota(jnp.int32, (BINS, BINS), 1)
    table = jnp.zeros((BINS, BINS), jnp.float32)
    for t in range(powers):
        first = t * slots
        log_ref[pl.ds(t, 1), :] = logs[pl.ds(first + mine, 1), :]
        away = pair_sum(
            [
                jnp.minimum(jnp.abs(places[pl.ds(first + m, 1), :] - levels), 1.0)
                for m in range(slots)
            ]
        )
        table = jnp.where(lane == t, jnp.sum(slots - away, axis=1, keepdims=True), table)
    hist_ref[...] = table.T[:powers]


def histogram(panel_bits, powers, conn, other, scale):
    genes = conn.shape[1]
    return pl.pallas_call(
        functools.partial(hist_kernel, scale, panel_bits),
        out_shape=(
            pltpu.VMEM((powers, genes), jnp.float32),
            pltpu.VMEM((powers, BINS), jnp.float32),
        ),
        in_specs=[VMEM, VMEM],
        out_specs=(VMEM, VMEM),
        scratch_shapes=[pltpu.VMEM(conn.shape, jnp.float32)] * 2,
        compiler_params=PARAMS,
        name="histogram",
    )(in_vmem(conn), in_vmem(other))


def fit_kernel(log_total, hist_ref, other_ref, fit_ref, slope_ref):
    hist = hist_ref[...] + other_ref[...]
    powers = hist.shape[0]
    lane = lax.broadcasted_iota(jnp.int32, (powers, BINS), 1)
    centers = lane.astype(jnp.float32) * (log_total / (BINS - 1))

    def total(x):
        return jnp.sum(x, axis=1, keepdims=True)

    weight_sum = total(hist)
    ylog = jnp.log(hist + 1.0) - log_total
    xdev = centers - total(hist * centers) / weight_sum
    ydev = ylog - total(hist * ylog) / weight_sum
    sxx = jnp.maximum(total(hist * xdev * xdev) / weight_sum, 0.05)
    syy = jnp.maximum(total(hist * ydev * ydev) / weight_sum, 0.05)
    sxy = total(hist * xdev * ydev) / weight_sum
    own = lax.broadcasted_iota(jnp.int32, (powers, BINS), 0) == lane

    def store(ref, column):
        ref[...] = jnp.sum(jnp.where(own, column, 0.0), axis=0)[:powers]

    store(fit_ref, -sxy * jnp.abs(sxy) / (sxx * syy))
    store(slope_ref, sxy / sxx)


def scale_free_fit(hist, other, log_total):
    powers = hist.shape[0]
    return pl.pallas_call(
        functools.partial(fit_kernel, log_total),
        out_shape=(jax.ShapeDtypeStruct((powers,), jnp.float32),) * 2,
        in_specs=[VMEM, VMEM],
        out_specs=(VMEM, VMEM),
        compiler_params=PARAMS,
        name="scale_free_fit",
    )(in_vmem(hist), in_vmem(other))


def on_device(expression, power_order):
    rows, cols = lax.axis_size("row"), lax.axis_size("col")
    count = rows * cols
    powers = power_order.shape[0]
    log_total = math.log(expression.shape[0] * count)
    panel_masks, partner_masks = plan(rows, cols)
    far, core = panel_masks[0], partner_masks[-1]
    low, sides = partner_masks[0], partner_masks[1:-1]

    partner = spread(expression, partner_masks, count)
    panel = spread(expression, panel_masks, count)
    keys = list(panel)
    front = [k for k in keys if not k & far & ~core] + [far]
    rear = [k for k in keys if k not in front]

    panel_bits = [mask & ~core for mask in panel_masks]

    relayed = [k for k in partner if bin(k & ~core).count("1") > 1]
    near = [k for k in keys if not k & far]
    waves = [
        ([0], [0]),
        (near, [core]),
        (near[1:], [0]),
        (near, sides),
        ([far], [0, core] + sides),
        (front, [low]),
        (front, [k ^ core for k in sides] + [low ^ core]),
        (front, [k for k in relayed if not k & core]),
        (front, [k for k in relayed if k & core][:-1]),
    ]
    tail = [k for k in relayed if k & core][-1]
    done = []
    parts = {k: [] for k in keys}
    for n, (panels, partners) in enumerate(wave for wave in waves if wave[1]):
        done.append(power_sums([panel[k] for k in panels], [partner[k] for k in partners], powers))
        for i, k in enumerate(panels):
            parts[k].append((n, i))
    everyone = [k for k in partner if k != tail]
    early, late = everyone[CHUNK:], everyone[:CHUNK]
    if early:
        done.append(power_sums([panel[k] for k in rear], [partner[k] for k in early], powers))
    for i, k in enumerate(rear):
        parts[k] += [(len(done) - 1, i)] * bool(early) + [(REAR, i)]
    for i, k in enumerate(front + rear):
        parts[k].append((FRONT, i))
    conn = last_sums(
        panel_bits,
        power_order,
        [panel[k] for k in front + rear],
        partner[tail],
        [panel[k] for k in rear],
        [partner[k] for k in late],
        done,
        [parts[k] for k in keys],
    )

    for mask in panel_masks[:0:-1]:
        conn = conn + swap(conn, mask, count)
    log_conn, hist = histogram(
        panel_bits, powers, conn, swap(conn, far, count), (BINS - 1) / log_total
    )
    for mask in partner_masks[:-1]:
        hist = hist + swap(hist, (mask & ~core) ^ core, count)
    fit, slope = scale_free_fit(hist, swap(hist, core, count), log_total)
    return (log_conn.T, fit, slope)


def solution(mesh):
    placed = (P(AXES, None), P())
    return jax.shard_map(
        on_device,
        mesh=mesh,
        in_specs=placed,
        out_specs=(P(AXES, None), P(), P()),
        check_vma=False,
    )
```

```python
import functools
import math

import jax
import jax.numpy as jnp
from jax import lax
from jax.experimental import pallas as pl
from jax.experimental.pallas import tpu as pltpu
from jax.sharding import PartitionSpec as P


AXES = ("row", "col")
BINS = 128
CHUNK = 8
FRONT, REAR = -1, -2
VMEM = pl.BlockSpec(memory_space=pltpu.VMEM)
SMEM = pl.BlockSpec(memory_space=pltpu.SMEM)
PARAMS = pltpu.CompilerParams(vmem_limit_bytes=16 * 2**20)


def swap(x, mask, count):
    return lax.ppermute(x, AXES, [(i, i ^ mask) for i in range(count)])


def spread(block, masks, count):
    held = {0: block}
    for mask in masks:
        for key in list(held):
            held[key ^ mask] = swap(held[key], mask, count)
    return held


def plan(rows, cols):
    row_masks = [cols << i for i in range(rows.bit_length() - 1)]
    core, *col_masks = [1 << i for i in range(cols.bit_length() - 1)]
    panel_masks = [row_masks[-1]] + col_masks
    partner_masks = row_masks[-2::-1] + [core]
    return panel_masks, partner_masks


def in_vmem(x):
    return pltpu.with_memory_space_constraint(x, pltpu.VMEM)


def pair_sum(values):
    while len(values) > 1:
        values = [a + b for a, b in zip(values[::2], values[1::2])]
    return values[0]


def joined(refs):
    return refs[0][...] if len(refs) == 1 else jnp.concatenate([r[...] for r in refs], axis=0)


def add_powers(panel_refs, partner_refs, total_ref):
    genes, samples = panel_refs[0].shape
    powers = total_ref.shape[1]
    panel = joined(panel_refs)
    many = len(panel_refs) > 1
    groups = [partner_refs] if many else [[ref] for ref in partner_refs]
    begun = False
    for group in groups:
        corr = lax.dot_general(
            joined(group), panel, (((1,), (1,)), ((), ())), preferred_element_type=jnp.float32
        )
        for low in range(0, corr.shape[0], genes):
            for i in range(len(panel_refs)):
                block = corr[low : low + genes, i * genes : (i + 1) * genes]
                magnitude = jnp.abs(block * (1.0 / samples))
                square = magnitude * magnitude
                current = [magnitude, square]
                for power in range(powers):
                    part = jnp.sum(current[power % 2].reshape(-1, 8, genes), axis=0)
                    total_ref[i, power] = total_ref[i, power] + part if begun else part
                    if power + 2 < powers:
                        current[power % 2] = current[power % 2] * square
            begun = True


def power_kernel(n_panel, *refs):
    out_ref, total_ref = refs[-2:]
    add_powers(refs[:n_panel], refs[n_panel:-2], total_ref)
    for i in range(n_panel):
        out_ref[i] = jnp.sum(total_ref[i], axis=1)


def power_sums(panels, partners, powers):
    genes, samples = panels[0].shape
    outs = []
    for first in range(0, len(partners), CHUNK):
        some = partners[first : first + CHUNK]
        flops = len(panels) * len(some) * genes * genes * 2 * samples
        outs.append(
            pl.pallas_call(
                functools.partial(power_kernel, len(panels)),
                out_shape=jax.ShapeDtypeStruct((len(panels), powers, genes), jnp.float32),
                in_specs=[VMEM] * (len(panels) + len(some)),
                out_specs=VMEM,
                scratch_shapes=[pltpu.VMEM((len(panels), powers, 8, genes), jnp.float32)],
                compiler_params=PARAMS,
                cost_estimate=pl.CostEstimate(flops=flops, bytes_accessed=0, transcendentals=0),
                name="power_sums",
            )(*map(in_vmem, panels), *map(in_vmem, some))
        )
    return functools.reduce(jnp.add, outs)


def own_slot(panel_bits):
    index = lax.axis_index("row") * lax.axis_size("col") + lax.axis_index("col")
    return sum(((index // bit) % 2) << i for i, bit in enumerate(panel_bits))


def last_kernel(panel_bits, n_front, n_panel, n_partner, parts, order_hbm, *refs):
    front_refs, tail_ref, refs = refs[:n_front], refs[n_front], refs[n_front + 1 :]
    part_refs = refs[n_panel + n_partner : -6]
    conn_ref, front_total, total_ref, natural, order, arrived = refs[-6:]
    slots = len(parts)
    powers = total_ref.shape[1]
    fetch = pltpu.make_async_copy(order_hbm, order, arrived)
    fetch.start()
    mine = own_slot(panel_bits)
    for i, where in enumerate(parts):
        values = [part_refs[a][b] for a, b in where if a >= 0]
        if values:
            natural[i] = functools.reduce(jnp.add, values)
    add_powers(front_refs, [tail_ref], front_total)
    add_powers(refs[:n_panel], refs[n_panel : n_panel + n_partner], total_ref)
    for i, where in enumerate(parts):
        values = [natural[i]] if any(a >= 0 for a, _ in where) else []
        values += [jnp.sum(front_total[b], axis=1) for a, b in where if a == FRONT]
        values += [jnp.sum(total_ref[b], axis=1) for a, b in where if a == REAR]
        natural[i] = functools.reduce(jnp.add, values)
    fetch.wait()
    for t in range(powers):
        at = order[t]
        for i in range(slots):
            slot = jnp.bitwise_xor(mine, i)
            conn_ref[pl.ds(t * slots + slot, 1), :] = natural[i, pl.ds(at, 1), :]


def last_sums(panel_bits, power_order, front, tail, panels, partners, done, parts):
    genes, samples = panels[0].shape
    powers = power_order.shape[0]
    flops = len(panels) * len(partners) * genes * genes * 2 * samples
    return pl.pallas_call(
        functools.partial(
            last_kernel, panel_bits, len(front), len(panels), len(partners), parts
        ),
        out_shape=jax.ShapeDtypeStruct((powers * len(parts), genes), jnp.float32),
        in_specs=[pl.BlockSpec(memory_space=pltpu.HBM)]
        + [VMEM] * (len(front) + 1 + len(panels) + len(partners) + len(done)),
        out_specs=VMEM,
        scratch_shapes=[
            pltpu.VMEM((len(front), powers, 8, genes), jnp.float32),
            pltpu.VMEM((len(panels), powers, 8, genes), jnp.float32),
            pltpu.VMEM((len(parts), powers, genes), jnp.float32),
            pltpu.SMEM((powers,), jnp.int32),
            pltpu.SemaphoreType.DMA(()),
        ],
        compiler_params=PARAMS,
        cost_estimate=pl.CostEstimate(flops=flops, bytes_accessed=0, transcendentals=0),
        name="last_sums",
    )(power_order, *map(in_vmem, [*front, tail, *panels, *partners, *done]))


def hist_kernel(scale, panel_bits, conn_ref, other_ref, log_ref, hist_ref, logs, places):
    rows, genes = conn_ref.shape
    powers = log_ref.shape[0]
    slots = rows // powers
    mine = own_slot(panel_bits)
    logs[...] = jnp.log(conn_ref[...] + other_ref[...])
    places[...] = logs[...] * scale
    levels = lax.broadcasted_iota(jnp.int32, (BINS, genes), 0).astype(jnp.float32)
    lane = lax.broadcasted_iota(jnp.int32, (BINS, BINS), 1)
    table = jnp.zeros((BINS, BINS), jnp.float32)
    for t in range(powers):
        first = t * slots
        log_ref[pl.ds(t, 1), :] = logs[pl.ds(first + mine, 1), :]
        away = pair_sum(
            [
                jnp.minimum(jnp.abs(places[pl.ds(first + m, 1), :] - levels), 1.0)
                for m in range(slots)
            ]
        )
        table = jnp.where(lane == t, jnp.sum(slots - away, axis=1, keepdims=True), table)
    hist_ref[...] = table.T[:powers]


def histogram(panel_bits, powers, conn, other, scale):
    genes = conn.shape[1]
    return pl.pallas_call(
        functools.partial(hist_kernel, scale, panel_bits),
        out_shape=(
            pltpu.VMEM((powers, genes), jnp.float32),
            pltpu.VMEM((powers, BINS), jnp.float32),
        ),
        in_specs=[VMEM, VMEM],
        out_specs=(VMEM, VMEM),
        scratch_shapes=[pltpu.VMEM(conn.shape, jnp.float32)] * 2,
        compiler_params=PARAMS,
        name="histogram",
    )(in_vmem(conn), in_vmem(other))


def fit_kernel(log_total, hist_ref, other_ref, fit_ref, slope_ref):
    hist = hist_ref[...] + other_ref[...]
    powers = hist.shape[0]
    lane = lax.broadcasted_iota(jnp.int32, (powers, BINS), 1)
    centers = lane.astype(jnp.float32) * (log_total / (BINS - 1))

    def total(x):
        return jnp.sum(x, axis=1, keepdims=True)

    share = 1.0 / total(hist)
    ylog = jnp.log(hist + 1.0) - log_total
    xdev = centers - total(hist * centers) * share
    ydev = ylog - total(hist * ylog) * share
    sxx = jnp.maximum(total(hist * xdev * xdev) * share, 0.05)
    syy = jnp.maximum(total(hist * ydev * ydev) * share, 0.05)
    sxy = total(hist * xdev * ydev) * share
    own = lax.broadcasted_iota(jnp.int32, (powers, BINS), 0) == lane

    def store(ref, column):
        ref[...] = jnp.sum(jnp.where(own, column, 0.0), axis=0)[:powers]

    store(fit_ref, -sxy * jnp.abs(sxy) / (sxx * syy))
    store(slope_ref, sxy / sxx)


def scale_free_fit(hist, other, log_total):
    powers = hist.shape[0]
    return pl.pallas_call(
        functools.partial(fit_kernel, log_total),
        out_shape=(jax.ShapeDtypeStruct((powers,), jnp.float32),) * 2,
        in_specs=[VMEM, VMEM],
        out_specs=(VMEM, VMEM),
        compiler_params=PARAMS,
        name="scale_free_fit",
    )(in_vmem(hist), in_vmem(other))


def on_device(expression, power_order):
    rows, cols = lax.axis_size("row"), lax.axis_size("col")
    count = rows * cols
    powers = power_order.shape[0]
    log_total = math.log(expression.shape[0] * count)
    panel_masks, partner_masks = plan(rows, cols)
    far, core = panel_masks[0], partner_masks[-1]
    low, sides = partner_masks[0], partner_masks[1:-1]

    partner = spread(expression, partner_masks, count)
    panel = spread(expression, panel_masks, count)
    keys = list(panel)
    front = [k for k in keys if not k & far & ~core] + [far]
    rear = [k for k in keys if k not in front]

    panel_bits = [mask & ~core for mask in panel_masks]

    relayed = [k for k in partner if bin(k & ~core).count("1") > 1]
    waves = [
        ([0], [0]),
        (front, [core] + sides),
        (front[1:], [0]),
        (front, [k ^ core for k in sides] + [low, low ^ core]),
        (front, [k for k in relayed if not k & core]),
        (front, [k for k in relayed if k & core][:-1]),
    ]
    tail = [k for k in relayed if k & core][-1]
    done = []
    parts = {k: [] for k in keys}
    for n, (panels, partners) in enumerate(wave for wave in waves if wave[1]):
        done.append(power_sums([panel[k] for k in panels], [partner[k] for k in partners], powers))
        for i, k in enumerate(panels):
            parts[k].append((n, i))
    everyone = list(partner)
    early, late = everyone[CHUNK:], everyone[:CHUNK]
    if early:
        done.append(power_sums([panel[k] for k in rear], [partner[k] for k in early], powers))
    for i, k in enumerate(rear):
        parts[k] += [(len(done) - 1, i)] * bool(early) + [(REAR, i)]
    for i, k in enumerate(front):
        parts[k].append((FRONT, i))
    conn = last_sums(
        panel_bits,
        power_order,
        [panel[k] for k in front],
        partner[tail],
        [panel[k] for k in rear],
        [partner[k] for k in late],
        done,
        [parts[k] for k in keys],
    )

    for mask in panel_masks[:0:-1]:
        conn = conn + swap(conn, mask, count)
    log_conn, hist = histogram(
        panel_bits, powers, conn, swap(conn, far, count), (BINS - 1) / log_total
    )
    for mask in partner_masks[:-1]:
        hist = hist + swap(hist, (mask & ~core) ^ core, count)
    fit, slope = scale_free_fit(hist, swap(hist, core, count), log_total)
    return (log_conn.T, fit, slope)


def solution(mesh):
    placed = (P(AXES, None), P())
    return jax.shard_map(
        on_device,
        mesh=mesh,
        in_specs=placed,
        out_specs=(P(AXES, None), P(), P()),
        check_vma=False,
    )
```
